32 devices in a mesh: cuts: 4 (over z), dp: 4 (over y, x), mp: 2 (over core).
Axes of the slice: x: 2, y: 2, z: 4, core: 2. Of those that a mesh axis runs over, the one named last changes fastest.
Arguments:
- attn_out: bfloat16 [2048, 3072], P(('cuts', 'dp'), 'mp'), may hold values from -6 to 6
- out_weight: bfloat16 [3072, 6144], P('mp'), may hold values from -0.109375 to 0.109375
- residual: bfloat16 [2048, 6144], P(('cuts', 'dp', 'mp')), may hold values from -45 to 45
- target: bfloat16 [2048, 6144], P(('cuts', 'dp', 'mp')), may hold values from -5 to 5
- norm_gain: float32 [6144], replicated, may hold values from 0.1 to 1.9
Outputs:
- block_out: bfloat16 [2048, 6144], P(('cuts', 'dp', 'mp'))
- attn_grad: bfloat16 [2048, 3072], P(('cuts', 'dp'), 'mp')
- weight_grad: float32 [3072, 6144], P('mp', 'dp')
The draws below stay inside these ranges and needn't reach their ends.
All inputs are finite; a program needn't handle non-finite values.
Results may differ from the reference program's by a relative error of at most 0.018.
Values may be sent and summed in bfloat16 or wider, within the bound.
A program may use at most 128 MiB of HBM per device.

```python
import math
import jax
import jax.numpy as jnp
from jax import lax

D = 6144
TOK_DEV = 128
INNER = 3072
REPLICAS = 16
TOKENS = 2048
N_MP = 2


def draw_residual(key, part):
    key_rows = jax.random.fold_in(key, 11)
    key_cols = jax.random.fold_in(key, 12)
    key_base = jax.random.fold_in(key, 13)
    row_scale = jnp.exp(jax.random.uniform(key_rows, (TOKENS, 1), jnp.float32, math.log(0.3), math.log(3.0)))
    col_scale = jnp.exp(jax.random.uniform(key_cols, (1, D), jnp.float32, math.log(0.3), math.log(3.0)))
    base = jnp.clip(jax.random.normal(key_base, (TOKENS, D), jnp.float32), -5.0, 5.0)
    return (base * row_scale * col_scale).astype(jnp.bfloat16)


def draw_target(key, part):
    key_base = jax.random.fold_in(key, 21)
    key_offset = jax.random.fold_in(key, 22)
    offset = jax.random.uniform(key_offset, (TOKENS, 1), jnp.float32, -1.0, 1.0)
    base = jnp.clip(jax.random.normal(key_base, (TOKENS, D), jnp.float32), -4.0, 4.0)
    return (base + offset).astype(jnp.bfloat16)


def level_of(rng, extent, pieces, least, largest):
    level, own = 1.0, jax.random.fold_in(rng, 6)
    for position, shards_of in pieces:
        draws = jnp.exp(jax.random.uniform(jax.random.fold_in(own, position), (shards_of,), jnp.float32, least / len(pieces), largest / len(pieces)))
        level = level * jnp.repeat(draws, extent[position] // shards_of).reshape([-1 if axis == position else 1 for axis in range(len(extent))])
    return level


def scatter_about(stream_key, shape, width, limit, pieces=(), kind=jnp.bfloat16):
    gain = level_of(stream_key, shape, pieces, -0.22, 0.18) if pieces else 1.0
    array = jax.random.normal(stream_key, shape, jnp.float32) * width * gain
    return jnp.minimum(jnp.maximum(array, -limit), limit).astype(kind)


def setup_inputs(seed: int = 0) -> dict:
    seeds = jax.random.split(jax.random.key(seed), 6)
    return {
        "attn_out": scatter_about(seeds[0], (TOKENS, INNER), 1.0, 6.0, ((0, 16), (1, 2))),
        "out_weight": scatter_about(seeds[1], (INNER, D), INNER ** -0.5, 0.109375, ((0, 2),)),
        "residual": draw_residual(jax.random.fold_in(seeds[5], 71), 0),
        "target": draw_target(jax.random.fold_in(seeds[5], 71), 0),
        "norm_gain": jnp.clip(1.0 + 0.18 * jax.random.normal(seeds[4], (D,), jnp.float32), 0.1, 1.9),
    }


epsilon = 1e-06

def norm_backward(stream, target, norm_gain):
    center = stream - lax.optimization_barrier(jnp.mean(stream, axis=1, keepdims=True))
    inv_std = lax.rsqrt(lax.optimization_barrier(jnp.mean(center * center, axis=1, keepdims=True)) + epsilon)
    normed = center * inv_std
    misfit = normed * norm_gain[None, :] - target.astype(jnp.float32)
    gain_err = misfit * norm_gain[None, :]
    bracket = gain_err - lax.optimization_barrier(jnp.mean(gain_err, axis=1, keepdims=True)) - normed * lax.optimization_barrier(jnp.mean(gain_err * normed, axis=1, keepdims=True))
    return (inv_std * bracket).astype(jnp.bfloat16)

def reference(attn_out, out_weight, residual, target, norm_gain):
    group_cols = INNER // N_MP
    replica_scale = 1.0 / REPLICAS
    heads_all = attn_out.reshape(REPLICAS, TOK_DEV, INNER)
    resid_all = residual.reshape(REPLICAS, TOK_DEV, D)
    target_all = target.reshape(REPLICAS, TOK_DEV, D)

    def replica_step(grad_sum, inputs):
        head_block, resid_block, target_block = inputs
        stream = resid_block.astype(jnp.float32)
        for group_idx in range(N_MP):
            low = group_idx * group_cols
            partial_value = jnp.dot(head_block[:, low:low + group_cols], out_weight[low:low + group_cols], preferred_element_type=jnp.float32)
            stream = stream + lax.optimization_barrier(partial_value.astype(jnp.bfloat16)).astype(jnp.float32)
        cotangent = norm_backward(stream, target_block, norm_gain)
        attn_rows = lax.dot_general(cotangent, out_weight, (((1,), (1,)), ((), ())), preferred_element_type=jnp.float32).astype(jnp.bfloat16)
        shares = lax.dot_general(head_block, cotangent, (((0,), (0,)), ((), ())), preferred_element_type=jnp.float32) * replica_scale
        grad_sum = grad_sum + lax.optimization_barrier(shares.astype(jnp.bfloat16)).astype(jnp.float32)
        return (grad_sum, (stream.astype(jnp.bfloat16), attn_rows))
    grad_sum, outputs = lax.scan(replica_step, jnp.zeros((INNER, D), jnp.float32), (heads_all, resid_all, target_all))
    block_out, attn_grad = outputs
    return (block_out.reshape(TOKENS, D), attn_grad.reshape(TOKENS, INNER), grad_sum)
```

```python
import functools

import jax
import jax.numpy as jnp
from jax import lax
from jax.experimental import pallas as pl
from jax.experimental.pallas import tpu as pltpu
from jax.sharding import PartitionSpec as P

epsilon = 1e-06


def norm_backward(stream, target, norm_gain):
    center = stream - jnp.mean(stream, axis=1, keepdims=True)
    inv_std = lax.rsqrt(jnp.mean(center * center, axis=1, keepdims=True) + epsilon)
    normed = center * inv_std
    misfit = normed * norm_gain[None, :] - target.astype(jnp.float32)
    gain_err = misfit * norm_gain[None, :]
    bracket = (
        gain_err
        - jnp.mean(gain_err, axis=1, keepdims=True)
        - normed * jnp.mean(gain_err * normed, axis=1, keepdims=True)
    )
    return (inv_std * bracket).astype(jnp.bfloat16)


def per_device(attn_out, out_weight, residual, target, norm_gain):
    tokens_dev = attn_out.shape[0]
    head_cols = attn_out.shape[1]
    replica_scale = 1.0 / (lax.axis_size("cuts") * lax.axis_size("dp"))
    summed = lax.psum_scatter(
        jnp.dot(attn_out, out_weight, preferred_element_type=jnp.float32).astype(jnp.bfloat16),
        "mp",
        scatter_dimension=0,
        tiled=True,
    ).astype(jnp.float32)
    stream = summed + residual.astype(jnp.float32)
    block_out = stream.astype(jnp.bfloat16)
    cotangent = norm_backward(stream, target, norm_gain)
    portion = lax.all_gather(cotangent, "mp", axis=0, tiled=True)
    stored = portion
    act_acc = lax.dot_general(
        portion, out_weight, (((1,), (1,)), ((), ())), preferred_element_type=jnp.float32
    )
    collected, act_acc = (stored, act_acc)
    attn_grad = act_acc.astype(jnp.bfloat16)
    columns = lax.all_to_all(collected, "dp", split_axis=1, concat_axis=0, tiled=True)
    column_width = columns.shape[1]
    portion = lax.all_gather(attn_out, "dp", axis=0, tiled=True)
    blocks_in = portion.shape[0] // tokens_dev
    head_block = portion.reshape(blocks_in, tokens_dev, head_cols)
    column_part = columns.reshape(blocks_in, tokens_dev, column_width)
    shares = (
        jnp.einsum("bti,btj->bij", head_block, column_part, preferred_element_type=jnp.float32)
        * replica_scale
    )
    rounded = lax.optimization_barrier(shares.astype(jnp.bfloat16))
    grad_block = jnp.sum(rounded.astype(jnp.float32), axis=0)
    weight_grad = lax.psum(grad_block.astype(jnp.bfloat16), "cuts").astype(jnp.float32)
    return (block_out, attn_grad, weight_grad)


MESH = pl.DeviceIdType.MESH


def remote(src, dst, send_sem, recv_sem, **where):
    return pltpu.make_async_remote_copy(
        src_ref=src, dst_ref=dst, send_sem=send_sem, recv_sem=recv_sem, device_id=where, device_id_type=MESH
    )


def fused(
    nz, ndp, chunk, attn_h, w_h, res_h, tgt_h, gain_h, blk_o, agrad_o, wgrad_o,
    w_v, a_v, rows_v, cot_v, part, part_in, res_v, tgt_v, gain_v, blk_v, agrad_v, acc,
    ld_s, w_s, p_s, p_r, au_s, ad_s, az_r, ap_s, ap_r, cp_s, cq_s, cq_r, cu_s, cd_s, c_r, ce_s, ce_r, o_s,
):
    z, dp, m = lax.axis_index("cuts"), lax.axis_index("dp"), lax.axis_index("mp")
    other = 1 - m
    tok, heads = attn_h.shape
    half, width = res_h.shape
    cols = width // ndp
    chunks = width // chunk
    has_up, has_down = z + 1 < nz, z >= 1
    scale = 1.0 / (nz * ndp)

    loads = [
        pltpu.make_async_copy(attn_h, a_v.at[z, dp], ld_s.at[0]),
        pltpu.make_async_copy(res_h, res_v, ld_s.at[1]),
        pltpu.make_async_copy(tgt_h, tgt_v, ld_s.at[2]),
        pltpu.make_async_copy(gain_h, gain_v, ld_s.at[3]),
    ]
    loads[0].start()

    def w_load(c):
        at = pl.ds(pl.multiple_of(c * chunk, chunk), chunk)
        return pltpu.make_async_copy(w_h.at[:, at], w_v.at[:, at], w_s.at[c])

    for c in range(chunks):
        w_load(c).start()
    for load in loads[1:]:
        load.start()

    barrier = pltpu.get_barrier_semaphore()
    pl.semaphore_signal(barrier, inc=1, device_id={"mp": other}, device_id_type=MESH)
    for k in range(1, ndp):
        pl.semaphore_signal(barrier, inc=1, device_id={"dp": lax.rem(dp + k, ndp)}, device_id_type=MESH)

    @pl.when(has_up)
    def _():
        pl.semaphore_signal(barrier, inc=1, device_id={"cuts": z + 1}, device_id_type=MESH)

    @pl.when(has_down)
    def _():
        pl.semaphore_signal(barrier, inc=1, device_id={"cuts": z - 1}, device_id_type=MESH)

    pl.semaphore_wait(barrier, ndp + jnp.where(has_up, 1, 0) + jnp.where(has_down, 1, 0))

    def a_up(l):
        return remote(a_v.at[l, dp], a_v.at[l, dp], au_s.at[l], az_r.at[l], cuts=z + 1)

    def a_down(l):
        return remote(a_v.at[l, dp], a_v.at[l, dp], ad_s.at[l], az_r.at[l], cuts=z - 1)

    def a_plane(l, k):
        return remote(a_v.at[l, dp], a_v.at[l, dp], ap_s.at[l, k], ap_r.at[l, dp], dp=lax.rem(dp + k, ndp))

    def a_plane_in(l, k):
        src = lax.rem(dp + ndp - k, ndp)
        return remote(a_v.at[l, src], a_v.at[l, src], ap_s.at[l, k], ap_r.at[l, src], dp=src)

    def c_up(l, d, src=None):
        return remote(cot_v.at[l, d, m] if src is None else src, cot_v.at[l, d, m], cu_s.at[l, d], c_r.at[l, d], cuts=z + 1)

    def c_down(l, d, src=None):
        return remote(cot_v.at[l, d, m] if src is None else src, cot_v.at[l, d, m], cd_s.at[l, d], c_r.at[l, d], cuts=z - 1)

    def c_pair(l, d):
        return remote(cot_v.at[l, d, m], cot_v.at[l, d, m], ce_s.at[l, d], ce_r.at[l, d], mp=other)

    def c_pair_in(l, d):
        return remote(cot_v.at[l, d, other], cot_v.at[l, d, other], ce_s.at[l, d], ce_r.at[l, d], mp=other)

    def a_hop(k):
        low, high = z - k, z + k

        @pl.when(low >= 0)
        def _():
            a_up(low).wait_recv()

            @pl.when(has_up)
            def _():
                a_up(low).start()

        @pl.when(high < nz)
        def _():
            a_down(high).wait_recv()

            @pl.when(has_down)
            def _():
                a_down(high).start()

    def both(k, f):
        pl.when(z - k >= 0)(lambda: f(z - k))
        pl.when(z + k < nz)(lambda: f(z + k))

    loads[0].wait()

    @pl.when(has_up)
    def _():
        a_up(z).start()

    @pl.when(has_down)
    def _():
        a_down(z).start()

    for k in range(1, ndp):
        a_plane(z, k).start()

    def p_send(c):
        at = pl.ds(pl.multiple_of(c * chunk, chunk), chunk)
        return remote(part.at[other, :, at], part_in.at[:, at], p_s.at[c], p_r.at[c], mp=other)

    @pl.loop(0, chunks)
    def _(c):
        at = pl.ds(pl.multiple_of(c * chunk, chunk), chunk)
        w_load(c).wait()
        value = jnp.dot(a_v[z, dp], w_v[:, at], preferred_element_type=jnp.float32).astype(jnp.bfloat16)
        part[0, :, at] = value[:half]
        part[1, :, at] = value[half:]
        p_send(c).start()

    a_hop(1)
    for load in loads[1:]:
        load.wait()

    @pl.loop(0, chunks)
    def _(c):
        p_send(c).wait()

    step = 16
    gain = gain_v[...]

    @pl.loop(0, half // step)
    def _(i):
        at = pl.ds(pl.multiple_of(i * step, step), step)
        stream = (
            part[m, at, :].astype(jnp.float32) + part_in[at, :].astype(jnp.float32) + res_v[at, :].astype(jnp.float32)
        )
        blk_v[at, :] = stream.astype(jnp.bfloat16)
        center = stream - jnp.mean(stream, axis=1, keepdims=True)
        inv_std = lax.rsqrt(jnp.mean(center * center, axis=1, keepdims=True) + epsilon)
        normed = center * inv_std
        gain_err = (normed * gain - tgt_v[at, :].astype(jnp.float32)) * gain
        bracket = (
            gain_err
            - jnp.mean(gain_err, axis=1, keepdims=True)
            - normed * jnp.mean(gain_err * normed, axis=1, keepdims=True)
        )
        cot = (inv_std * bracket).astype(jnp.bfloat16)
        for d in range(ndp):
            rows_v[d, m, at, :] = cot[:, d * cols : (d + 1) * cols]

    def c_plane(k):
        to = lax.rem(dp + k, ndp)
        return remote(rows_v.at[to, m], cot_v.at[z, dp, m], cp_s.at[k], c_r.at[z, dp], dp=to)

    def c_rows():
        return remote(rows_v.at[:, m], rows_v.at[:, m], cq_s.at[0], cq_r.at[0], mp=other)

    def c_rows_in():
        return remote(rows_v.at[:, other], rows_v.at[:, other], cq_s.at[0], cq_r.at[0], mp=other)

    for k in range(1, ndp):
        c_plane(k).start()
    own = rows_v.at[dp, m]

    @pl.when(has_up)
    def _():
        c_up(z, dp, own).start()

    @pl.when(has_down)
    def _():
        c_down(z, dp, own).start()

    c_rows().start()
    blk_copy = pltpu.make_async_copy(blk_v, blk_o, ld_s.at[1])
    blk_copy.start()
    cot_v[z, dp, m] = rows_v[dp, m]

    both(1, lambda l: [a_plane(l, k).start() for k in range(1, ndp)] and None)
    c_rows_in().wait_recv()
    cot_v[z, dp, other] = rows_v[dp, other]

    def c_forward(l, d, up, down):
        pl.when(up)(lambda: c_up(l, d).start())
        pl.when(down)(lambda: c_down(l, d).start())
        c_pair(l, d).start()

    for k in range(1, ndp):
        d = lax.rem(dp + ndp - k, ndp)
        c_up(z, d).wait_recv()
        c_forward(z, d, has_up, has_down)
    for k in range(2, nz):
        a_hop(k)
        both(k, lambda l: [a_plane(l, j).start() for j in range(1, ndp)] and None)

    tile = 512 if heads % 512 == 0 else heads

    @pl.loop(0, heads // tile)
    def _(j):
        at = pl.ds(pl.multiple_of(j * tile, tile), tile)
        total = jnp.zeros((tok, tile), jnp.float32)
        for d in range(ndp):
            total += lax.dot_general(
                rows_v[d].reshape(tok, cols), w_v[at, d * cols : (d + 1) * cols], (((1,), (1,)), ((), ())),
                preferred_element_type=jnp.float32,
            )
        agrad_v[:, at] = total.astype(jnp.bfloat16)

    agrad_copy = pltpu.make_async_copy(agrad_v, agrad_o, ld_s.at[2])
    agrad_copy.start()

    wide = 256 if heads % 256 == 0 else heads

    def group(l, first):
        for k in range(1, ndp):
            a_plane_in(l, k).wait_recv()

        @pl.loop(0, heads // wide)
        def _(j):
            at = pl.ds(pl.multiple_of(j * wide, wide), wide)
            value = scale * lax.dot_general(
                a_v[l, :, :, at].reshape(ndp * tok, wide), cot_v[l].reshape(ndp * tok, cols), (((0,), (0,)), ((), ())),
                preferred_element_type=jnp.float32,
            )
            acc[at, :] = value if first else acc[at, :] + value

    for k in range(1, ndp):
        c_pair_in(z, lax.rem(dp + ndp - k, ndp)).wait_recv()
    group(z, True)

    @pl.loop(1, nz)
    def _(k):
        for j in range(ndp):
            d = lax.rem(dp + ndp - j, ndp)

            @pl.when(z - k >= 0)
            def _():
                c_up(z - k, d).wait_recv()
                c_forward(z - k, d, has_up, False)

            @pl.when(z + k < nz)
            def _():
                c_down(z + k, d).wait_recv()
                c_forward(z + k, d, False, has_down)

        def finish(l):
            for j in range(ndp):
                c_pair_in(l, j).wait_recv()
            group(l, False)

        both(k, finish)

    out = pltpu.make_async_copy(acc, wgrad_o, o_s.at[0])
    out.start()

    @pl.loop(0, nz)
    def _(l):
        @pl.when(has_up & (l <= z))
        def _():
            a_up(l).wait_send()
            for d in range(ndp):
                c_up(l, d).wait_send()

        @pl.when(has_down & (l >= z))
        def _():
            a_down(l).wait_send()
            for d in range(ndp):
                c_down(l, d).wait_send()

        for k in range(1, ndp):
            a_plane(l, k).wait_send()
            c_pair(l, lax.rem(dp + k, ndp)).wait_send()

        @pl.when(l != z)
        def _():
            c_pair(l, dp).wait_send()

    for k in range(1, ndp):
        c_plane(k).wait_send()
    c_rows().wait_send()
    blk_copy.wait()
    agrad_copy.wait()
    out.wait()


def fused_device(nz, ndp, attn_out, out_weight, residual, target, norm_gain):
    tok, heads = attn_out.shape
    half, width = residual.shape
    cols = width // ndp
    chunk = 512 if width % 512 == 0 else 128
    chunks = width // chunk
    bf16, f32 = jnp.bfloat16, jnp.float32
    dma = pltpu.SemaphoreType.DMA
    any_space = pl.BlockSpec(memory_space=pl.ANY)
    return pl.pallas_call(
        functools.partial(fused, nz, ndp, chunk),
        out_shape=(
            jax.ShapeDtypeStruct((half, width), bf16),
            jax.ShapeDtypeStruct((tok, heads), bf16),
            jax.ShapeDtypeStruct((heads, cols), f32),
        ),
        in_specs=[any_space] * 5,
        out_specs=(any_space,) * 3,
        scratch_shapes=[
            pltpu.VMEM((heads, width), bf16),
            pltpu.VMEM((nz, ndp, tok, heads), bf16),
            pltpu.VMEM((ndp, 2, half, cols), bf16),
            pltpu.VMEM((nz, ndp, 2, half, cols), bf16),
            pltpu.VMEM((2, half, width), bf16),
            pltpu.VMEM((half, width), bf16),
            pltpu.VMEM((half, width), bf16),
            pltpu.VMEM((half, width), bf16),
            pltpu.VMEM((1, width), f32),
            pltpu.VMEM((half, width), bf16),
            pltpu.VMEM((tok, heads), bf16),
            pltpu.VMEM((heads, cols), f32),
            dma((4,)), dma((chunks,)), dma((chunks,)), dma((chunks,)),
            dma((nz,)), dma((nz,)), dma((nz,)), dma((nz, ndp)), dma((nz, ndp)),
            dma((ndp,)), dma((1,)), dma((1,)),
            dma((nz, ndp)), dma((nz, ndp)), dma((nz, ndp)), dma((nz, ndp)), dma((nz, ndp)), dma((1,)),
        ],
        compiler_params=pltpu.CompilerParams(
            collective_id=0, has_side_effects=True, vmem_limit_bytes=66 * 1000 * 1000
        ),
    )(attn_out, out_weight, residual, target, norm_gain.reshape(1, width))


def solution(mesh):
    if mesh.shape["mp"] == 2:
        body = functools.partial(fused_device, mesh.shape["cuts"], mesh.shape["dp"])
    else:
        body = per_device
    placed = (
        P(("cuts", "dp"), "mp"),
        P("mp", None),
        P(("cuts", "dp", "mp"), None),
        P(("cuts", "dp", "mp"), None),
        P(),
    )
    return jax.shard_map(
        body,
        mesh=mesh,
        in_specs=placed,
        out_specs=(P(("cuts", "dp", "mp"), None), P(("cuts", "dp"), "mp"), P("mp", "dp")),
        check_vma=False,
    )
```

```python
import functools

import jax
import jax.numpy as jnp
from jax import lax
from jax.experimental import pallas as pl
from jax.experimental.pallas import tpu as pltpu
from jax.sharding import PartitionSpec as P

epsilon = 1e-06


def norm_backward(stream, target, norm_gain):
    center = stream - jnp.mean(stream, axis=1, keepdims=True)
    inv_std = lax.rsqrt(jnp.mean(center * center, axis=1, keepdims=True) + epsilon)
    normed = center * inv_std
    misfit = normed * norm_gain[None, :] - target.astype(jnp.float32)
    gain_err = misfit * norm_gain[None, :]
    bracket = (
        gain_err
        - jnp.mean(gain_err, axis=1, keepdims=True)
        - normed * jnp.mean(gain_err * normed, axis=1, keepdims=True)
    )
    return (inv_std * bracket).astype(jnp.bfloat16)


def per_device(attn_out, out_weight, residual, target, norm_gain):
    tokens_dev = attn_out.shape[0]
    head_cols = attn_out.shape[1]
    replica_scale = 1.0 / (lax.axis_size("cuts") * lax.axis_size("dp"))
    summed = lax.psum_scatter(
        jnp.dot(attn_out, out_weight, preferred_element_type=jnp.float32).astype(jnp.bfloat16),
        "mp",
        scatter_dimension=0,
        tiled=True,
    ).astype(jnp.float32)
    stream = summed + residual.astype(jnp.float32)
    block_out = stream.astype(jnp.bfloat16)
    cotangent = norm_backward(stream, target, norm_gain)
    portion = lax.all_gather(cotangent, "mp", axis=0, tiled=True)
    stored = portion
    act_acc = lax.dot_general(
        portion, out_weight, (((1,), (1,)), ((), ())), preferred_element_type=jnp.float32
    )
    collected, act_acc = (stored, act_acc)
    attn_grad = act_acc.astype(jnp.bfloat16)
    columns = lax.all_to_all(collected, "dp", split_axis=1, concat_axis=0, tiled=True)
    column_width = columns.shape[1]
    portion = lax.all_gather(attn_out, "dp", axis=0, tiled=True)
    blocks_in = portion.shape[0] // tokens_dev
    head_block = portion.reshape(blocks_in, tokens_dev, head_cols)
    column_part = columns.reshape(blocks_in, tokens_dev, column_width)
    shares = (
        jnp.einsum("bti,btj->bij", head_block, column_part, preferred_element_type=jnp.float32)
        * replica_scale
    )
    rounded = lax.optimization_barrier(shares.astype(jnp.bfloat16))
    grad_block = jnp.sum(rounded.astype(jnp.float32), axis=0)
    weight_grad = lax.psum(grad_block.astype(jnp.bfloat16), "cuts").astype(jnp.float32)
    return (block_out, attn_grad, weight_grad)


MESH = pl.DeviceIdType.MESH


def remote(src, dst, send_sem, recv_sem, **where):
    return pltpu.make_async_remote_copy(
        src_ref=src, dst_ref=dst, send_sem=send_sem, recv_sem=recv_sem, device_id=where, device_id_type=MESH
    )


def fused(
    nz, ndp, chunk, attn_h, w_h, res_h, tgt_h, gain_h, blk_o, agrad_o, wgrad_o,
    w_v, a_v, rows_v, cot_v, part, part_in, res_v, tgt_v, gain_v, blk_v, agrad_v, acc, out_v,
    ld_s, w_s, p_s, p_r, au_s, ad_s, az_r, ap_s, ap_r, cp_s, cq_s, cq_r, cu_s, cd_s, c_r, ce_s, ce_r, o_s,
):
    z, dp, m = lax.axis_index("cuts"), lax.axis_index("dp"), lax.axis_index("mp")
    other = 1 - m
    tok, heads = attn_h.shape
    half, width = res_h.shape
    cols = width // ndp
    chunks = width // chunk
    has_up, has_down = z + 1 < nz, z >= 1
    scale = 1.0 / (nz * ndp)

    loads = [
        pltpu.make_async_copy(attn_h, a_v.at[z, dp], ld_s.at[0]),
        pltpu.make_async_copy(res_h, res_v, ld_s.at[1]),
        pltpu.make_async_copy(tgt_h, tgt_v, ld_s.at[2]),
        pltpu.make_async_copy(gain_h, gain_v, ld_s.at[3]),
    ]
    loads[0].start()

    def w_load(c):
        at = pl.ds(pl.multiple_of(c * chunk, chunk), chunk)
        return pltpu.make_async_copy(w_h.at[:, at], w_v.at[:, at], w_s.at[c])

    for c in range(chunks):
        w_load(c).start()
    for load in loads[1:]:
        load.start()

    barrier = pltpu.get_barrier_semaphore()
    pl.semaphore_signal(barrier, inc=1, device_id={"mp": other}, device_id_type=MESH)
    for k in range(1, ndp):
        pl.semaphore_signal(barrier, inc=1, device_id={"dp": lax.rem(dp + k, ndp)}, device_id_type=MESH)

    @pl.when(has_up)
    def _():
        pl.semaphore_signal(barrier, inc=1, device_id={"cuts": z + 1}, device_id_type=MESH)

    @pl.when(has_down)
    def _():
        pl.semaphore_signal(barrier, inc=1, device_id={"cuts": z - 1}, device_id_type=MESH)

    pl.semaphore_wait(barrier, ndp + jnp.where(has_up, 1, 0) + jnp.where(has_down, 1, 0))

    def a_up(l):
        return remote(a_v.at[l, dp], a_v.at[l, dp], au_s.at[l], az_r.at[l], cuts=z + 1)

    def a_down(l):
        return remote(a_v.at[l, dp], a_v.at[l, dp], ad_s.at[l], az_r.at[l], cuts=z - 1)

    def a_plane(l, k):
        return remote(a_v.at[l, dp], a_v.at[l, dp], ap_s.at[l, k], ap_r.at[l, dp], dp=lax.rem(dp + k, ndp))

    def a_plane_in(l, k):
        src = lax.rem(dp + ndp - k, ndp)
        return remote(a_v.at[l, src], a_v.at[l, src], ap_s.at[l, k], ap_r.at[l, src], dp=src)

    def c_up(l, d, src=None):
        return remote(cot_v.at[l, d, m] if src is None else src, cot_v.at[l, d, m], cu_s.at[l, d], c_r.at[l, d], cuts=z + 1)

    def c_down(l, d, src=None):
        return remote(cot_v.at[l, d, m] if src is None else src, cot_v.at[l, d, m], cd_s.at[l, d], c_r.at[l, d], cuts=z - 1)

    def c_pair(l, d):
        return remote(cot_v.at[l, d, m], cot_v.at[l, d, m], ce_s.at[l, d], ce_r.at[l, d], mp=other)

    def c_pair_in(l, d):
        return remote(cot_v.at[l, d, other], cot_v.at[l, d, other], ce_s.at[l, d], ce_r.at[l, d], mp=other)

    def a_hop(k):
        low, high = z - k, z + k

        @pl.when(low >= 0)
        def _():
            a_up(low).wait_recv()

            @pl.when(has_up)
            def _():
                a_up(low).start()

        @pl.when(high < nz)
        def _():
            a_down(high).wait_recv()

            @pl.when(has_down)
            def _():
                a_down(high).start()

    def both(k, f):
        pl.when(z - k >= 0)(lambda: f(z - k))
        pl.when(z + k < nz)(lambda: f(z + k))

    loads[0].wait()

    @pl.when(has_up)
    def _():
        a_up(z).start()

    @pl.when(has_down)
    def _():
        a_down(z).start()

    for k in range(1, ndp):
        a_plane(z, k).start()

    def p_send(c):
        at = pl.ds(pl.multiple_of(c * chunk, chunk), chunk)
        return remote(part.at[other, :, at], part_in.at[:, at], p_s.at[c], p_r.at[c], mp=other)

    @pl.loop(0, chunks)
    def _(c):
        at = pl.ds(pl.multiple_of(c * chunk, chunk), chunk)
        w_load(c).wait()
        value = jnp.dot(a_v[z, dp], w_v[:, at], preferred_element_type=jnp.float32).astype(jnp.bfloat16)
        part[0, :, at] = value[:half]
        part[1, :, at] = value[half:]
        p_send(c).start()

    a_hop(1)
    for load in loads[1:]:
        load.wait()

    @pl.loop(0, chunks)
    def _(c):
        p_send(c).wait()

    step = 16
    gain = gain_v[...]

    @pl.loop(0, half // step)
    def _(i):
        at = pl.ds(pl.multiple_of(i * step, step), step)
        stream = (
            part[m, at, :].astype(jnp.float32) + part_in[at, :].astype(jnp.float32) + res_v[at, :].astype(jnp.float32)
        )
        blk_v[at, :] = stream.astype(jnp.bfloat16)
        center = stream - jnp.mean(stream, axis=1, keepdims=True)
        inv_std = lax.rsqrt(jnp.mean(center * center, axis=1, keepdims=True) + epsilon)
        normed = center * inv_std
        gain_err = (normed * gain - tgt_v[at, :].astype(jnp.float32)) * gain
        bracket = (
            gain_err
            - jnp.mean(gain_err, axis=1, keepdims=True)
            - normed * jnp.mean(gain_err * normed, axis=1, keepdims=True)
        )
        cot = (inv_std * bracket).astype(jnp.bfloat16)
        for d in range(ndp):
            rows_v[d, m, at, :] = cot[:, d * cols : (d + 1) * cols]

    def c_plane(k):
        to = lax.rem(dp + k, ndp)
        return remote(rows_v.at[to, m], cot_v.at[z, dp, m], cp_s.at[k], c_r.at[z, dp], dp=to)

    def c_rows():
        return remote(rows_v.at[:, m], rows_v.at[:, m], cq_s.at[0], cq_r.at[0], mp=other)

    def c_rows_in():
        return remote(rows_v.at[:, other], rows_v.at[:, other], cq_s.at[0], cq_r.at[0], mp=other)

    for k in range(1, ndp):
        c_plane(k).start()
    own = rows_v.at[dp, m]

    @pl.when(has_up)
    def _():
        c_up(z, dp, own).start()

    @pl.when(has_down)
    def _():
        c_down(z, dp, own).start()

    c_rows().start()
    blk_copy = pltpu.make_async_copy(blk_v, blk_o, ld_s.at[1])
    blk_copy.start()
    cot_v[z, dp, m] = rows_v[dp, m]

    both(1, lambda l: [a_plane(l, k).start() for k in range(1, ndp)] and None)
    c_rows_in().wait_recv()
    cot_v[z, dp, other] = rows_v[dp, other]

    def c_forward(l, d, up, down):
        pl.when(up)(lambda: c_up(l, d).start())
        pl.when(down)(lambda: c_down(l, d).start())
        c_pair(l, d).start()

    for k in range(1, ndp):
        d = lax.rem(dp + ndp - k, ndp)
        c_up(z, d).wait_recv()
        c_forward(z, d, has_up, has_down)
    for k in range(2, nz):
        a_hop(k)
        both(k, lambda l: [a_plane(l, j).start() for j in range(1, ndp)] and None)

    tile = 512 if heads % 512 == 0 else heads

    @pl.loop(0, heads // tile)
    def _(j):
        at = pl.ds(pl.multiple_of(j * tile, tile), tile)
        total = jnp.zeros((tok, tile), jnp.float32)
        for d in range(ndp):
            total += lax.dot_general(
                rows_v[d].reshape(tok, cols), w_v[at, d * cols : (d + 1) * cols], (((1,), (1,)), ((), ())),
                preferred_element_type=jnp.float32,
            )
        agrad_v[:, at] = total.astype(jnp.bfloat16)

    agrad_copy = pltpu.make_async_copy(agrad_v, agrad_o, ld_s.at[2])
    agrad_copy.start()

    wide = 256 if heads % 256 == 0 else heads

    far = jnp.maximum(z, nz - 1 - z)

    def out_copy(j):
        at = pl.ds(pl.multiple_of(j * wide, wide), wide)
        return pltpu.make_async_copy(out_v.at[at, :], wgrad_o.at[at, :], o_s.at[j])

    def group(l, first, last):
        for k in range(1, ndp):
            a_plane_in(l, k).wait_recv()

        @pl.loop(0, heads // wide)
        def _(j):
            at = pl.ds(pl.multiple_of(j * wide, wide), wide)
            value = scale * lax.dot_general(
                a_v[l, :, :, at].reshape(ndp * tok, wide), cot_v[l].reshape(ndp * tok, cols), (((0,), (0,)), ((), ())),
                preferred_element_type=jnp.float32,
            )
            value = value if first else acc[at, :] + value
            acc[at, :] = value

            @pl.when(last)
            def _():
                out_v[at, :] = value.astype(jnp.bfloat16)
                out_copy(j).start()

    for k in range(1, ndp):
        c_pair_in(z, lax.rem(dp + ndp - k, ndp)).wait_recv()
    group(z, True, far == 0)

    @pl.loop(1, nz)
    def _(k):
        for j in range(ndp):
            d = lax.rem(dp + ndp - j, ndp)

            @pl.when(z - k >= 0)
            def _():
                c_up(z - k, d).wait_recv()
                c_forward(z - k, d, has_up, False)

            @pl.when(z + k < nz)
            def _():
                c_down(z + k, d).wait_recv()
                c_forward(z + k, d, False, has_down)

        def finish(l):
            for j in range(ndp):
                c_pair_in(l, j).wait_recv()
            group(l, False, (l == z + far) | ((l == z - far) & (z + far >= nz)))

        both(k, finish)

    @pl.loop(0, nz)
    def _(l):
        @pl.when(has_up & (l <= z))
        def _():
            a_up(l).wait_send()
            for d in range(ndp):
                c_up(l, d).wait_send()

        @pl.when(has_down & (l >= z))
        def _():
            a_down(l).wait_send()
            for d in range(ndp):
                c_down(l, d).wait_send()

        for k in range(1, ndp):
            a_plane(l, k).wait_send()
            c_pair(l, lax.rem(dp + k, ndp)).wait_send()

        @pl.when(l != z)
        def _():
            c_pair(l, dp).wait_send()

    for k in range(1, ndp):
        c_plane(k).wait_send()
    c_rows().wait_send()
    blk_copy.wait()
    agrad_copy.wait()

    @pl.loop(0, heads // wide)
    def _(j):
        out_copy(j).wait()


def widen(blk_i, agrad_i, wgrad_i, blk_o, agrad_o, wgrad_o):
    blk_o[...] = blk_i[...]
    agrad_o[...] = agrad_i[...]
    wgrad_o[...] = wgrad_i[...].astype(jnp.float32)


def fused_device(nz, ndp, attn_out, out_weight, residual, target, norm_gain):
    tok, heads = attn_out.shape
    half, width = residual.shape
    cols = width // ndp
    chunk = 512 if width % 512 == 0 else 128
    chunks = width // chunk
    tiles = heads // 256 if heads % 256 == 0 else 1
    bf16, f32 = jnp.bfloat16, jnp.float32
    dma = pltpu.SemaphoreType.DMA
    any_space = pl.BlockSpec(memory_space=pl.ANY)
    blk, agrad, wgrad = pl.pallas_call(
        functools.partial(fused, nz, ndp, chunk),
        out_shape=(
            jax.ShapeDtypeStruct((half, width), bf16),
            jax.ShapeDtypeStruct((tok, heads), bf16),
            jax.ShapeDtypeStruct((heads, cols), bf16),
        ),
        in_specs=[any_space] * 5,
        out_specs=(any_space,) * 3,
        scratch_shapes=[
            pltpu.VMEM((heads, width), bf16),
            pltpu.VMEM((nz, ndp, tok, heads), bf16),
            pltpu.VMEM((ndp, 2, half, cols), bf16),
            pltpu.VMEM((nz, ndp, 2, half, cols), bf16),
            pltpu.VMEM((2, half, width), bf16),
            pltpu.VMEM((half, width), bf16),
            pltpu.VMEM((half, width), bf16),
            pltpu.VMEM((half, width), bf16),
            pltpu.VMEM((1, width), f32),
            pltpu.VMEM((half, width), bf16),
            pltpu.VMEM((tok, heads), bf16),
            pltpu.VMEM((heads, cols), f32),
            pltpu.VMEM((heads, cols), bf16),
            dma((4,)), dma((chunks,)), dma((chunks,)), dma((chunks,)),
            dma((nz,)), dma((nz,)), dma((nz,)), dma((nz, ndp)), dma((nz, ndp)),
            dma((ndp,)), dma((1,)), dma((1,)),
            dma((nz, ndp)), dma((nz, ndp)), dma((nz, ndp)), dma((nz, ndp)), dma((nz, ndp)), dma((tiles,)),
        ],
        compiler_params=pltpu.CompilerParams(
            collective_id=0, has_side_effects=True, vmem_limit_bytes=66 * 1000 * 1000
        ),
    )(attn_out, out_weight, residual, target, norm_gain.reshape(1, width))
    parts = tiles if width % (tiles * 128) == 0 and heads % (tiles * 128) == 0 else 1
    specs = [
        pl.BlockSpec((half, width // parts), lambda i: (0, i)),
        pl.BlockSpec((tok, heads // parts), lambda i: (0, i)),
        pl.BlockSpec((heads // parts, cols), lambda i: (i, 0)),
    ]
    return pl.pallas_call(
        widen,
        grid=(parts,),
        out_shape=(
            jax.ShapeDtypeStruct((half, width), bf16),
            jax.ShapeDtypeStruct((tok, heads), bf16),
            jax.ShapeDtypeStruct((heads, cols), f32),
        ),
        in_specs=specs,
        out_specs=tuple(specs),
        compiler_params=pltpu.CompilerParams(vmem_limit_bytes=32 * 1000 * 1000),
    )(blk, agrad, wgrad)


def solution(mesh):
    if mesh.shape["mp"] == 2:
        body = functools.partial(fused_device, mesh.shape["cuts"], mesh.shape["dp"])
    else:
        body = per_device
    placed = (
        P(("cuts", "dp"), "mp"),
        P("mp", None),
        P(("cuts", "dp", "mp"), None),
        P(("cuts", "dp", "mp"), None),
        P(),
    )
    return jax.shard_map(
        body,
        mesh=mesh,
        in_specs=placed,
        out_specs=(P(("cuts", "dp", "mp"), None), P(("cuts", "dp"), "mp"), P("mp", "dp")),
        check_vma=False,
    )
```
